32 devices in a mesh: blk: 8 (over z, x), ga: 4 (over y, core).
Axes of the slice: x: 2, y: 2, z: 4, core: 2. Of those that a mesh axis runs over, the one named last changes fastest.
Arguments:
- pair_val: bfloat16 [16, 16, 16, 2048], P('blk', None, None, 'ga'), may hold values from -0.125 to 0.125
- pair_con: bfloat16 [16, 16, 16, 2048], P('blk', None, None, 'ga'), may hold values from -6 to 6
- screened: bfloat16 [16, 2048, 2048], P('blk', None, 'ga'), may hold values from -0.125 to 0.125
- amplitude: bfloat16 [16, 16], P('blk'), may hold values from -6 to 6
- qmap: int32 [16, 16], P('blk'), may hold values from 0 to 15, as said below
Outputs:
- kernel_x: float32 [16, 16], P('blk')
The draws below stay inside these ranges and needn't reach their ends.
Inputs may be any that keep to these rules, and one draw needn't show every extreme that they name: qmap[k, k'] is the label of the difference k - k' (periodic) on a grid of 8 by 2 points, with the points and the differences labelled at random; every row and every column holds each label once.
All inputs are finite; a program needn't handle non-finite values.
Results may differ from the reference program's by a relative error of at most 0.004.
Values may be sent and summed in bfloat16 or wider, within the bound.
No kernel may reach another device: no remote copies, remote signals or barrier semaphores. Data moves between devices by JAX's collectives and lax.ppermute only.
A program may use at most 64 MiB of HBM per device.

```python
import jax
import jax.numpy as jnp
from jax import lax

NV = 4
NC = 4
NG = 2048
GRID_X = 8
NK = 16


def draw_qmap(key, part):
    point_order = jax.random.permutation(jax.random.fold_in(key, 11), NK)
    label_order = jax.random.permutation(jax.random.fold_in(key, 23), NK)
    rows_y = NK // GRID_X
    coord_x = point_order % GRID_X
    coord_y = point_order // GRID_X
    diff_x = (coord_x[:, None] - coord_x[None, :]) % GRID_X
    diff_y = (coord_y[:, None] - coord_y[None, :]) % rows_y
    return label_order[diff_y * GRID_X + diff_x].astype(jnp.int32)


def block_scale(own_key, shape, shards, smallest, high):
    factor_of, own = 1.0, jax.random.fold_in(own_key, 6)
    for dim, shards_of in shards:
        steps = jnp.exp(jax.random.uniform(jax.random.fold_in(own, dim), (shards_of,), jnp.float32, smallest / len(shards), high / len(shards)))
        factor_of = factor_of * jnp.repeat(steps, shape[dim] // shards_of).reshape([-1 if axis == dim else 1 for axis in range(len(shape))])
    return factor_of


def bell_draw(stream_key, shape, width, reach, pieces=(), held_as=jnp.bfloat16):
    values = width * jax.random.normal(stream_key, shape, jnp.float32)
    if pieces:
        values = values * block_scale(stream_key, shape, pieces, -0.22, 0.18)
    return jnp.clip(values, -reach, reach).astype(held_as)


def setup_inputs(seed: int = 0) -> dict:
    key_list = jax.random.split(jax.random.key(seed), 6)
    return {
        "pair_val": bell_draw(key_list[0], (NK, NK, NV * NV, NG), NG ** -0.5, 0.125, ((0, 8), (3, 4))),
        "pair_con": bell_draw(key_list[1], (NK, NK, NC * NC, NG), 1.0, 6.0, ((0, 8), (3, 4))),
        "screened": bell_draw(key_list[2], (NK, NG, NG), NG ** -0.5, 0.125, ((0, 8), (2, 4))),
        "amplitude": bell_draw(key_list[3], (NK, NV * NC), 1.0, 6.0, ((0, 8),)),
        "qmap": draw_qmap(jax.random.fold_in(key_list[5], 71), 0),
    }


def inverse_rows(qmap):
    total = qmap.shape[1]
    labels = jnp.arange(total, dtype=jnp.int32)
    hits = (qmap[:, :, None] == labels[None, None, :]).astype(jnp.int32)
    return jnp.sum(hits * labels[None, :, None], axis=1).astype(jnp.int32)


def reference(pair_val, pair_con, screened, amplitude, qmap):
    total = qmap.shape[0]
    partner = inverse_rows(qmap)
    rows = jnp.arange(total, dtype=jnp.int32)

    def per_label(label):
        chosen = lax.dynamic_index_in_dim(partner, label, 1, keepdims=False).astype(jnp.int32)
        values = pair_val[rows, chosen].astype(jnp.float32).reshape(total, NV, NV, NG)
        cons = pair_con[rows, chosen]
        amps = amplitude[chosen].astype(jnp.float32).reshape(total, NV, NC)
        zeta = jnp.einsum('navg,nvc->nacg', values, amps).astype(jnp.bfloat16)
        zeta = lax.optimization_barrier(zeta).astype(jnp.float32)
        weights = lax.dynamic_index_in_dim(screened, label, 0, keepdims=False)
        unit = jnp.dot(cons.reshape(total * NC * NC, NG), weights, preferred_element_type=jnp.float32).astype(jnp.bfloat16)
        unit = lax.optimization_barrier(unit).astype(jnp.float32).reshape(total, NC, NC, NG)
        return jnp.einsum('ncyg,nayg->nac', unit, zeta).reshape(total, NV * NC)

    parts = lax.map(per_label, rows)
    return jnp.sum(parts, 0) / total
```

```python
import jax
import jax.numpy as jnp
from jax import lax
from jax.sharding import PartitionSpec as P

NV = 4
NC = 4


def inverse_rows(qmap):
    total = qmap.shape[1]
    labels = jnp.arange(total, dtype=jnp.int32)
    hits = (qmap[:, :, None] == labels[None, None, :]).astype(jnp.int32)
    return jnp.sum(hits * labels[None, :, None], axis=1)


def swap(value, axis, size, step):
    return lax.ppermute(value, axis, [(i, i ^ step) for i in range(size)])


def body_of(blk, ga):
    def body(pair_val, pair_con, screened, amplitude, qmap):
        local_k, total, band_pairs, width = pair_val.shape
        local_q = screened.shape[0]
        slot = lax.axis_index("ga")
        every_amp = lax.all_gather(amplitude, "blk", axis=0, tiled=True)
        partner = inverse_rows(qmap)
        con_sorted = jnp.take_along_axis(pair_con, partner[:, :, None, None], axis=1)
        con_sorted, every_amp = lax.optimization_barrier((con_sorted, every_amp))
        con_in = lax.all_to_all(con_sorted, "blk", split_axis=1, concat_axis=0, tiled=True)

        val_sorted = jnp.take_along_axis(pair_val, partner[:, :, None, None], axis=1)
        amp_sorted = every_amp[partner].reshape(local_k, total, NV, NC)
        val_five = val_sorted.reshape(local_k, total, NV, NV, width)
        zeta = jnp.einsum("kqavg,kqvc->kqacg", val_five, amp_sorted, preferred_element_type=jnp.float32)
        zeta = zeta.astype(jnp.bfloat16).reshape(local_k, total, NV * NC, width)

        far = swap(con_in, "ga", ga, ga // 2)
        near = swap(con_in, "ga", ga, 1)
        zeta_in = lax.all_to_all(zeta, "blk", split_axis=1, concat_axis=0, tiled=True)
        pieces = {0: con_in, 1: near, ga // 2: far, ga // 2 + 1: swap(far, "ga", ga, 1)}
        weights = screened.reshape(local_q, ga, width, screened.shape[2])
        unit = 0.0
        for key, held in pieces.items():
            block = lax.dynamic_index_in_dim(weights, slot ^ key, 1, keepdims=False)
            unit = unit + jnp.einsum("kqxg,qgh->kqxh", held, block,
                                     preferred_element_type=jnp.float32)
        unit = unit.astype(jnp.bfloat16).reshape(total, local_q, NC, NC, -1)
        zeta = zeta_in.reshape(total, local_q, NV, NC, -1)
        terms = jnp.einsum("kqcyg,kqayg->kac", unit, zeta, preferred_element_type=jnp.float32)
        terms = terms.reshape(blk, 1, local_k, NV * NC)
        terms = jnp.broadcast_to(terms, (blk, ga, local_k, NV * NC)).reshape(blk * ga, local_k, NV * NC)
        back = lax.all_to_all(terms, ("blk", "ga"), split_axis=0, concat_axis=0, tiled=True)
        return jnp.sum(back, 0) / total
    return body


def solution(mesh):
    placed = (
        P("blk", None, None, "ga"),
        P("blk", None, None, "ga"),
        P("blk", None, "ga"),
        P("blk", None),
        P("blk", None),
    )
    return jax.shard_map(
        body_of(mesh.shape["blk"], mesh.shape["ga"]), mesh=mesh, in_specs=placed,
        out_specs=P("blk", None), check_vma=False
    )
```

```python
import jax
import jax.numpy as jnp
from jax import lax
from jax.sharding import PartitionSpec as P


NV = 4
NC = 4
EXTRA = 8


def inverse_rows(qmap):
    total = qmap.shape[1]
    labels = jnp.arange(total, dtype=jnp.int32)
    hits = (qmap[:, :, None] == labels[None, None, :]).astype(jnp.int32)
    return jnp.sum(hits * labels[None, :, None], axis=1)


def swap(value, axis, size, step):
    return lax.ppermute(value, axis, [(i, i ^ step) for i in range(size)])


def exchange(value):
    return lax.all_to_all(value, "blk", split_axis=0, concat_axis=0, tiled=True)


def body_of(blk, ga):
    def inner(pair_val, pair_con, screened, amplitude, qmap):
        local_k, total, band_pairs, width = pair_val.shape
        local_q = screened.shape[0]
        rows = local_q * local_k * band_pairs
        pairs = total * local_q
        slot = lax.axis_index("ga")
        partner = inverse_rows(qmap)

        by_dest = partner.reshape(local_k, blk, local_q).transpose(1, 2, 0)
        flat = (by_dest + total * jnp.arange(local_k, dtype=jnp.int32)).reshape(-1)
        con_rows = pair_con.reshape(local_k * total, band_pairs, width)[flat]
        val_rows = pair_val.reshape(local_k * total, band_pairs, width)[flat]

        note = jnp.concatenate([
            jnp.broadcast_to(amplitude.reshape(1, -1), (blk, amplitude.size)),
            by_dest.reshape(blk, -1).astype(jnp.bfloat16)], axis=1)
        assert note.shape[1] <= 128
        note = jnp.pad(note, ((0, 0), (0, 128 - note.shape[1])))
        note = jnp.broadcast_to(note[:, None, :], (blk, EXTRA, 128))
        tiles = rows * width // 128
        con_sent = con_rows.reshape(blk, rows // EXTRA, EXTRA, width // 128, 128)
        con_sent = con_sent.transpose(0, 1, 3, 2, 4).reshape(blk, tiles, 128)
        con_got = exchange(jnp.concatenate([con_sent, note], axis=1))
        val_in = exchange(val_rows.reshape(blk, rows, width))

        con_in = con_got[:, :tiles].reshape(blk, rows // EXTRA, width // 128, EXTRA, 128)
        con_in = con_in.transpose(0, 1, 3, 2, 4).reshape(blk, rows, width)
        note_in = con_got[:, tiles]
        count = amplitude.size
        every_amp = note_in[:, :count].reshape(total, NV * NC)
        whose = note_in[:, count:count + local_q * local_k].astype(jnp.int32)
        picks = (whose.reshape(pairs, 1) == jnp.arange(total, dtype=jnp.int32)[None, :])
        cp = jnp.arange(NC * NC * NV * NV) // (NV * NV) % NC
        vp = jnp.arange(NC * NC * NV * NV) % NV
        spread = (jnp.arange(NV * NC)[:, None] == (vp * NC + cp)[None, :]).astype(jnp.bfloat16)
        amp_of = jnp.dot(picks.astype(jnp.bfloat16), every_amp)
        factor = jnp.dot(amp_of, spread).astype(jnp.float32)
        factor = factor.reshape(blk, local_q, local_k, NC * NC, NV * NV)

        pieces = {0: con_in}
        step = ga // 2
        while step:
            pieces.update({key ^ step: swap(x, "ga", ga, step) for key, x in pieces.items()})
            step //= 2
        weights = screened.reshape(local_q, ga, width, screened.shape[2])
        unit = 0.0
        for key, held in pieces.items():
            block = lax.dynamic_index_in_dim(weights, slot ^ key, 1, keepdims=False)
            held = held.reshape(blk, local_q, local_k * band_pairs, width)
            unit = unit + jnp.einsum("bqxg,qgh->bqxh", held, block,
                                     preferred_element_type=jnp.float32)
        unit = unit.astype(jnp.bfloat16).reshape(blk, local_q, local_k, NC * NC, -1)
        val_in = val_in.reshape(blk, local_q, local_k, NV * NV, -1)
        cross = jnp.einsum("bqkxg,bqkyg->bqkxy", unit, val_in, preferred_element_type=jnp.float32)
        mixed = jnp.sum(cross * factor, axis=1)
        terms = mixed.reshape(blk, local_k, NC, NC, NV, NV).sum((3, 5))
        terms = terms.transpose(0, 1, 3, 2).reshape(blk, 1, local_k, NV * NC)
        terms = jnp.broadcast_to(terms, (blk, ga, local_k, NV * NC)).reshape(blk * ga, local_k, NV * NC)
        back = lax.all_to_all(terms, ("blk", "ga"), split_axis=0, concat_axis=0, tiled=True)
        return jnp.sum(back, 0) / total

    return inner


def solution(mesh):
    placed = (
        P("blk", None, None, "ga"),
        P("blk", None, None, "ga"),
        P("blk", None, "ga"),
        P("blk", None),
        P("blk", None),
    )
    return jax.shard_map(
        body_of(mesh.shape["blk"], mesh.shape["ga"]), mesh=mesh, in_specs=placed,
        out_specs=P("blk", None), check_vma=False
    )
```
